32 devices in a mesh: replica: 2 (over y), expert: 8 (over z, core), tensor: 2 (over x).
Axes of the slice: x: 2, y: 2, z: 4, core: 2. Of those that a mesh axis runs over, the one named last changes fastest.
Arguments:
- delta: bfloat16 [2, 128, 4, 14336], P('replica', 'expert', None, 'tensor'), may hold values from -6 to 6
- step_offsets: int32 [2], replicated, may hold values from 0 to 15, as said below
- block_map: int32 [128], replicated, may hold values from 0 to 127, as said below
- master_params: float32 [128, 4, 14336], P('expert', 'replica', 'tensor'), may hold values from -6 to 6
- first_moment: float32 [128, 4, 14336], P('expert', 'replica', 'tensor'), may hold values from -2 to 2
- second_moment: float32 [128, 4, 14336], P('expert', 'replica', 'tensor'), may hold values from 0.01 to 1
Outputs:
- new_params: bfloat16 [128, 4, 14336], P('expert', 'replica')
- new_first: float32 [128, 4, 14336], P('expert', 'replica', 'tensor')
- new_second: float32 [128, 4, 14336], P('expert', 'replica', 'tensor')
The draws below stay inside these ranges and needn't reach their ends.
Inputs may be any that keep to these rules, and one draw needn't show every extreme that they name: `block_map`: A permutation of the block indices onto owner slots; slot s belongs to expert index s // 16, and the blocks b with b // 16 = i go in equal numbers to every expert index. `step_offsets`: the replica groups' offsets are distinct.
All inputs are finite; a program needn't handle non-finite values.
Results may differ from the reference program's by a relative error of at most 0.0035.
Values may be sent and summed in bfloat16 or wider, within the bound.
A program may use at most 64 MiB of HBM per device.

```python
import math
import jax
import jax.numpy as jnp
from jax import lax

FF = 14336
BLK_DEV = 16
BR = 4
BLOCKS = 128
REPLICAS = 2


def shuffled(key_one):
    return jax.random.permutation(key_one, BLK_DEV)


def draw_block_map(key, part):
    owners = BLOCKS // BLK_DEV
    first_key = jax.random.fold_in(key, 11)
    second_key = jax.random.fold_in(key, 23)
    source_perm = jax.vmap(shuffled)(jax.random.split(first_key, owners)).astype(jnp.int32)
    target = source_perm % owners
    ordinal = source_perm // owners
    sources = jnp.arange(owners, dtype=jnp.int32)[:, None]
    arrival = sources * (BLK_DEV // owners) + ordinal
    owner_perm = jax.vmap(shuffled)(jax.random.split(second_key, owners)).astype(jnp.int32)
    slot_ids = owner_perm[target, arrival]
    return (target * BLK_DEV + slot_ids).reshape(BLOCKS).astype(jnp.int32)


def draw_step_offsets(key, part):
    inner_key = jax.random.fold_in(key, 37)
    order_key = jax.random.fold_in(key, 41)
    middle = jax.random.permutation(inner_key, jnp.arange(1, 15, dtype=jnp.int32))[:REPLICAS - 2]
    ends = jnp.array([0, 15], dtype=jnp.int32)
    values = jnp.concatenate([ends, middle.astype(jnp.int32)])
    return jax.random.permutation(order_key, values).astype(jnp.int32)


def spiked(drawn, stream_key, source, target, blocks, factor):
    owner, partner = [(jnp.arange(drawn.shape[position]) // (drawn.shape[position] // blocks)).reshape([-1 if axis == position else 1 for axis in range(drawn.ndim)]) for position in (source, target)]
    chosen = jax.random.permutation(stream_key, blocks)[partner]
    strong = (owner == chosen) | (owner == (partner + blocks // 2) % blocks)
    return jnp.where(strong, factor * drawn, drawn)


def shard_levels(own_key, shape, shards, low, high):
    factor_of = 1.0
    for axis_at, parts in shards:
        heights = jax.random.uniform(jax.random.fold_in(jax.random.fold_in(own_key, 6), axis_at), (parts,), jnp.float32, low / len(shards), high / len(shards))
        factor_of = factor_of * jnp.repeat(jnp.exp(heights), shape[axis_at] // parts).reshape((-1,) + (1,) * (len(shape) - 1 - axis_at))
    return factor_of


def noise(own_key, dims, scale, most, pieces=(), held_as=jnp.bfloat16):
    level = shard_levels(own_key, dims, pieces, -0.22, 0.18) if pieces else 1.0
    drawn = jax.random.normal(own_key, dims, jnp.float32) * scale * level
    return jnp.minimum(jnp.maximum(drawn, -most), most).astype(held_as)


def bell_draw_with(own_key, extent, width, limit, shards, heavy, held_as=jnp.bfloat16):
    values = width * jax.random.normal(own_key, extent, jnp.float32)
    if shards:
        values = values * shard_levels(own_key, extent, shards, -0.22, 0.18)
    return jnp.clip(spiked(values, jax.random.fold_in(own_key, 3), *heavy), -limit, limit).astype(held_as)


def setup_inputs(seed: int = 0) -> dict:
    key_list = jax.random.split(jax.random.key(seed), 7)
    return {
        "delta": bell_draw_with(key_list[0], (REPLICAS, BLOCKS, BR, FF), 1.0, 6.0, ((0, 2), (1, 8), (3, 2)), (0, 2, 2, 2.0)),
        "step_offsets": draw_step_offsets(jax.random.fold_in(key_list[6], 71), 0),
        "block_map": draw_block_map(jax.random.fold_in(key_list[6], 71), 0),
        "master_params": noise(key_list[3], (BLOCKS, BR, FF), 1.0, 6.0, ((0, 8), (1, 2), (2, 2)), jnp.float32),
        "first_moment": noise(key_list[4], (BLOCKS, BR, FF), 0.3, 2.0, ((0, 8), (1, 2), (2, 2)), jnp.float32),
        "second_moment": jnp.clip(jnp.exp(math.log(1.0) - 4.6051702 * jax.random.uniform(key_list[5], (BLOCKS, BR, FF), jnp.float32) ** shard_levels(key_list[5], (BLOCKS, BR, FF), ((0, 8), (1, 2), (2, 2)), -0.2, 0.2)), 0.01, 1.0),
    }


beta_one = 0.9
beta_two = 0.99
outer_rate = 0.7
outer_round = 20
epsilon = 1e-08

def replica_weights(step_offsets):
    reciprocal = 1.0 / (1.0 + step_offsets.astype(jnp.float32))
    return reciprocal / jnp.sum(reciprocal)

def adam_update(gradient, master_params, first_moment, second_moment):
    new_first = beta_one * first_moment + (1.0 - beta_one) * gradient
    new_second = beta_two * second_moment + (1.0 - beta_two) * gradient * gradient
    fix_one = 1.0 - beta_one ** outer_round
    fix_two = 1.0 - beta_two ** outer_round
    update_step = new_first / fix_one / (jnp.sqrt(new_second / fix_two) + epsilon)
    new_params = (master_params - outer_rate * update_step).astype(jnp.bfloat16)
    return (new_params, new_first, new_second)

def reference(delta, step_offsets, block_map, master_params, first_moment, second_moment):
    weights = replica_weights(step_offsets)

    def add_replica(replica_id, running):
        slice_rows = lax.dynamic_index_in_dim(delta, replica_id, 0, keepdims=False).astype(jnp.float32)
        scaled = (slice_rows * weights[replica_id]).astype(jnp.bfloat16)
        scaled = lax.optimization_barrier(scaled)
        return running + scaled.astype(jnp.float32)
    pseudo = lax.fori_loop(0, REPLICAS, add_replica, jnp.zeros(delta.shape[1:], jnp.float32))
    inverse = jnp.argsort(block_map).astype(jnp.int32)
    gradient = pseudo[inverse]
    new_params, new_first, new_second = adam_update(gradient, master_params, first_moment, second_moment)
    return (new_params, new_first, new_second)
```

```python
import functools

import jax
import jax.numpy as jnp
from jax import lax
from jax.experimental import pallas as pl
from jax.experimental.pallas import tpu as pltpu
from jax.sharding import PartitionSpec as P

beta_one = 0.9
beta_two = 0.99
outer_rate = 0.7
outer_round = 20
epsilon = 1e-08

LANES = 128
CHUNK = 8
LAG = 3
UNROLL = 4
MESH = pl.DeviceIdType.MESH


def kernel(
    sizes,
    block_map,
    step_offsets,
    delta,
    master_params,
    first_moment,
    second_moment,
    out_params,
    out_first,
    out_second,
    master,
    first,
    second,
    params,
    new_first,
    new_second,
    order,
    slots,
    places,
    load_sem,
    state_sem,
    own_sem,
    store_sem,
    y_send,
    y_recv,
    z_send,
    z_recv,
    x_send,
    x_recv,
    *buffers,
):
    replicas, experts, tensors, chunks, blocks, pairs, rows = sizes
    count = len(chunks)
    stage = buffers[:count]
    arrived = buffers[count : 2 * count]
    outgoing = buffers[2 * count : 3 * count]
    incoming = buffers[3 * count :]
    my_replica = lax.axis_index("replica")
    my_expert = lax.axis_index("expert")
    my_tensor = lax.axis_index("tensor")
    columns = sum(chunks)
    starts = [sum(chunks[:c]) for c in range(count)]

    def load(c, d):
        replica = lax.rem(my_replica + d, replicas)
        return pltpu.make_async_copy(
            delta.at[:, pl.ds(starts[c], chunks[c]), replica],
            stage[c].at[d],
            load_sem.at[c, d],
        )

    def y_copy(c, d):
        return pltpu.make_async_remote_copy(
            src_ref=stage[c].at[d],
            dst_ref=arrived[c].at[d - 1],
            send_sem=y_send.at[c, d],
            recv_sem=y_recv.at[c, d],
            device_id={"replica": lax.rem(my_replica + d, replicas)},
            device_id_type=MESH,
        )

    def z_copy(c, d):
        peer = lax.rem(my_expert + d, experts)
        return pltpu.make_async_remote_copy(
            src_ref=outgoing[c].at[pl.ds(peer * pairs, pairs)],
            dst_ref=incoming[c].at[pl.ds(my_expert * pairs, pairs)],
            send_sem=z_send.at[c, d],
            recv_sem=z_recv.at[c, d],
            device_id={"expert": peer},
            device_id_type=MESH,
        )

    def z_own(c):
        mine = pl.ds(my_expert * pairs, pairs)
        return pltpu.make_async_copy(outgoing[c].at[mine], incoming[c].at[mine], own_sem.at[c])

    def x_copy(c, d):
        part = params.at[:, pl.ds(my_tensor * columns + starts[c], chunks[c])]
        return pltpu.make_async_remote_copy(
            src_ref=part,
            dst_ref=part,
            send_sem=x_send.at[c, d],
            recv_sem=x_recv.at[c, d],
            device_id={"tensor": lax.rem(my_tensor + d, tensors)},
            device_id_type=MESH,
        )

    def store(c, which):
        held, out = ((new_first, out_first), (new_second, out_second))[which]
        part = pl.ds(starts[c] * rows, chunks[c] * rows)
        return pltpu.make_async_copy(held.at[:, part], out.at[:, part], store_sem.at[c, which])

    barrier = pltpu.get_barrier_semaphore()
    axes = (("replica", my_replica, replicas), ("expert", my_expert, experts), ("tensor", my_tensor, tensors))
    for axis, mine, size in axes:
        for d in range(1, size):
            pl.semaphore_signal(
                barrier, inc=1, device_id={axis: lax.rem(mine + d, size)}, device_id_type=MESH
            )
    for c in range(count):
        for d in list(range(1, replicas)) + [0]:
            load(c, d).start()
    states = [
        pltpu.make_async_copy(source, held, state_sem.at[i])
        for i, (source, held) in enumerate(
            ((master_params, master), (first_moment, first), (second_moment, second))
        )
    ]
    for copy in states:
        copy.start()

    def note_order(e, carry):
        seen = jnp.int32(0)
        found = [jnp.int32(0)] * pairs
        for j in range(blocks):
            owned = lax.div(block_map[my_expert * blocks + j], jnp.int32(blocks)) == e
            for k in range(pairs):
                found[k] = jnp.where(owned, jnp.where(seen == k, j, found[k]), found[k])
            seen = seen + jnp.where(owned, 1, 0)
        for k in range(pairs):
            order[e * pairs + k] = found[k]
        return carry

    def note_slots(i, carry):
        seen = jnp.int32(0)
        found = [jnp.int32(0)] * pairs
        for j in range(blocks):
            slot = block_map[i * blocks + j] - my_expert * blocks
            owned = jnp.where(slot >= 0, jnp.where(slot < blocks, 1, 0), 0)
            for k in range(pairs):
                found[k] = jnp.where(owned == 1, jnp.where(seen == k, slot, found[k]), found[k])
            seen = seen + owned
        for k in range(pairs):
            slots[i * pairs + k] = found[k]
        return carry

    def note_places(s, carry):
        place = jnp.int32(0)
        for q in range(blocks):
            place = jnp.where(slots[q] == s, q, place)
        places[s] = place
        return carry

    lax.fori_loop(0, experts, note_order, 0)
    lax.fori_loop(0, experts, note_slots, 0)
    lax.fori_loop(0, blocks, note_places, 0)

    pl.semaphore_wait(barrier, replicas + experts + tensors - 3)
    for c in range(count):
        for d in range(1, replicas):
            load(c, d).wait()
            y_copy(c, d).start()

    shares = [
        1.0 / jnp.full((8, LANES), 1 + step_offsets[lax.rem(my_replica + replicas - d, replicas)], jnp.int32).astype(jnp.float32)
        for d in range(replicas)
    ]
    total = functools.reduce(lambda a, b: a + b, shares)
    weights = [(share / total)[:1] for share in shares]

    fix_one = 1.0 - beta_one**outer_round
    fix_two = 1.0 - beta_two**outer_round

    def add_up(c):
        load(c, 0).wait()
        for d in range(1, replicas):
            y_copy(c, d).wait_recv()
        dense = chunks[c] * rows
        own = stage[c].reshape(replicas, blocks, dense, LANES)
        others = arrived[c].reshape(replicas - 1, blocks, dense, LANES)
        out = outgoing[c].reshape(blocks, dense, LANES)

        def step(n, carry):
            for u in range(UNROLL):
                p = n * UNROLL + u
                block = order[p]
                value = own[0, block].astype(jnp.float32) * weights[0]
                for d in range(1, replicas):
                    value = value + others[d - 1, block].astype(jnp.float32) * weights[d]
                out[p] = value.astype(jnp.bfloat16)
            return carry

        lax.fori_loop(0, blocks // UNROLL, step, 0)

    def adam(c):
        dense = chunks[c] * rows
        terms = incoming[c].reshape(blocks, dense, LANES)
        held = params.reshape(blocks, tensors * columns * rows, LANES)
        part = pl.ds(starts[c] * rows, dense)
        target = pl.ds(pl.multiple_of((my_tensor * columns + starts[c]) * rows, 16), dense)

        def step(n, carry):
            for u in range(UNROLL):
                s = n * UNROLL + u
                gradient = terms[places[s]].astype(jnp.float32)
                one = beta_one * first[s, part] + (1.0 - beta_one) * gradient
                two = beta_two * second[s, part] + (1.0 - beta_two) * gradient * gradient
                new_first[s, part] = one
                new_second[s, part] = two
                update = (outer_rate / fix_one) * one / (jnp.sqrt(two * (1.0 / fix_two)) + epsilon)
                held[s, target] = (master[s, part] - update).astype(jnp.bfloat16)
            return carry

        lax.fori_loop(0, blocks // UNROLL, step, 0)

    def finish(c):
        if c == 0:
            for copy in states:
                copy.wait()
        z_own(c).wait()
        for d in range(1, experts):
            z_copy(c, d).wait_recv()
        adam(c)
        for d in range(1, tensors):
            x_copy(c, d).start()
        for which in range(2):
            store(c, which).start()

    for c in range(count):
        add_up(c)
        for d in range(1, experts):
            z_copy(c, d).start()
        z_own(c).start()
        if c >= LAG:
            finish(c - LAG)
    for c in range(max(count - LAG, 0), count):
        finish(c)

    for c in range(count):
        for d in range(1, replicas):
            y_copy(c, d).wait_send()
        for d in range(1, experts):
            z_copy(c, d).wait_send()
        for which in range(2):
            store(c, which).wait()
    for c in range(count):
        for d in range(1, tensors):
            x_copy(c, d).wait()
    last = pltpu.make_async_copy(params, out_params, state_sem.at[0])
    last.start()
    last.wait()


def body(delta, step_offsets, block_map, master_params, first_moment, second_moment, *, shape):
    replicas, experts, tensors = shape
    blocks, rows_all, width = delta.shape[1:]
    rows = rows_all // replicas
    columns = width // LANES
    pairs = blocks // experts
    chunks = [CHUNK] * (columns // CHUNK)
    count = len(chunks)
    terms = delta.reshape(blocks, replicas, rows, columns, LANES).transpose(0, 3, 1, 2, 4)

    def dense(state):
        split = state.reshape(blocks, rows, columns, LANES).transpose(0, 2, 1, 3)
        return split.reshape(blocks, columns * rows, LANES)

    def undense(state):
        split = state.reshape(blocks, columns, rows, LANES).transpose(0, 2, 1, 3)
        return split.reshape(blocks, rows, width)

    state_shape = (blocks, columns * rows, LANES)
    params_shape = (blocks, tensors * columns, rows, LANES)
    anywhere = pl.BlockSpec(memory_space=pl.ANY)
    scalars = pl.BlockSpec(memory_space=pltpu.SMEM)
    dma = pltpu.SemaphoreType.DMA
    sizes = (replicas, experts, tensors, chunks, blocks, pairs, rows)
    new_params, new_first, new_second = pl.pallas_call(
        functools.partial(kernel, sizes),
        out_shape=(
            jax.ShapeDtypeStruct(params_shape, jnp.bfloat16),
            jax.ShapeDtypeStruct(state_shape, jnp.float32),
            jax.ShapeDtypeStruct(state_shape, jnp.float32),
        ),
        in_specs=[scalars] * 2 + [anywhere] * 4,
        out_specs=(anywhere,) * 3,
        scratch_shapes=[
            pltpu.VMEM(state_shape, jnp.float32),
            pltpu.VMEM(state_shape, jnp.float32),
            pltpu.VMEM(state_shape, jnp.float32),
            pltpu.VMEM(params_shape, jnp.bfloat16),
            pltpu.VMEM(state_shape, jnp.float32),
            pltpu.VMEM(state_shape, jnp.float32),
            pltpu.SMEM((blocks,), jnp.int32),
            pltpu.SMEM((blocks,), jnp.int32),
            pltpu.SMEM((blocks,), jnp.int32),
            dma((count, replicas)),
            dma((3,)),
            dma((count,)),
            dma((count, 2)),
            dma((count, replicas)),
            dma((count, replicas)),
            dma((count, experts)),
            dma((count, experts)),
            dma((count, tensors)),
            dma((count, tensors)),
        ]
        + [pltpu.VMEM((replicas, blocks, c, rows, LANES), jnp.bfloat16) for c in chunks]
        + [pltpu.VMEM((replicas - 1, blocks, c, rows, LANES), jnp.bfloat16) for c in chunks]
        + [pltpu.VMEM((blocks, c, rows, LANES), jnp.bfloat16) for c in chunks]
        + [pltpu.VMEM((blocks, c, rows, LANES), jnp.bfloat16) for c in chunks],
        compiler_params=pltpu.CompilerParams(collective_id=0, has_side_effects=True),
    )(block_map, step_offsets, terms, dense(master_params), dense(first_moment), dense(second_moment))
    full = new_params.transpose(0, 2, 1, 3).reshape(blocks, rows, tensors * width)
    return (full, undense(new_first), undense(new_second))


def solution(mesh):
    in_specs = (
        P("replica", "expert", None, "tensor"),
        P(),
        P(),
        P("expert", "replica", "tensor"),
        P("expert", "replica", "tensor"),
        P("expert", "replica", "tensor"),
    )
    out_specs = (
        P("expert", "replica", None),
        P("expert", "replica", "tensor"),
        P("expert", "replica", "tensor"),
    )
    shape = tuple(mesh.shape[axis] for axis in ("replica", "expert", "tensor"))
    step = functools.partial(body, shape=shape)
    return jax.shard_map(step, mesh=mesh, in_specs=in_specs, out_specs=out_specs, check_vma=False)
```

```python
import functools

import jax
import jax.numpy as jnp
from jax import lax
from jax.experimental import pallas as pl
from jax.experimental.pallas import tpu as pltpu
from jax.sharding import PartitionSpec as P

beta_one = 0.9
beta_two = 0.99
outer_rate = 0.7
outer_round = 20
epsilon = 1e-08

LANES = 128
CHUNK = 8
LAG = 3
UNROLL = 4
MESH = pl.DeviceIdType.MESH


def kernel(
    sizes,
    block_map,
    step_offsets,
    delta,
    master_params,
    first_moment,
    second_moment,
    params,
    new_first,
    new_second,
    master,
    first,
    second,
    order,
    slots,
    places,
    load_sem,
    state_sem,
    own_sem,
    y_send,
    y_recv,
    z_send,
    z_recv,
    x_send,
    x_recv,
    *buffers,
):
    replicas, experts, tensors, chunks, blocks, pairs, rows = sizes
    count = len(chunks)
    stage = buffers[:count]
    arrived = buffers[count : 2 * count]
    outgoing = buffers[2 * count : 3 * count]
    incoming = buffers[3 * count :]
    my_replica = lax.axis_index("replica")
    my_expert = lax.axis_index("expert")
    my_tensor = lax.axis_index("tensor")
    columns = sum(chunks)
    starts = [sum(chunks[:c]) for c in range(count)]

    def load(c, d):
        replica = lax.rem(my_replica + d, replicas)
        return pltpu.make_async_copy(
            delta.at[:, pl.ds(starts[c], chunks[c]), replica],
            stage[c].at[d],
            load_sem.at[c, d],
        )

    def y_copy(c, d):
        return pltpu.make_async_remote_copy(
            src_ref=stage[c].at[d],
            dst_ref=arrived[c].at[d - 1],
            send_sem=y_send.at[c, d],
            recv_sem=y_recv.at[c, d],
            device_id={"replica": lax.rem(my_replica + d, replicas)},
            device_id_type=MESH,
        )

    def z_copy(c, d):
        peer = lax.rem(my_expert + d, experts)
        return pltpu.make_async_remote_copy(
            src_ref=outgoing[c].at[pl.ds(peer * pairs, pairs)],
            dst_ref=incoming[c].at[pl.ds(my_expert * pairs, pairs)],
            send_sem=z_send.at[c, d],
            recv_sem=z_recv.at[c, d],
            device_id={"expert": peer},
            device_id_type=MESH,
        )

    def z_own(c):
        mine = pl.ds(my_expert * pairs, pairs)
        return pltpu.make_async_copy(outgoing[c].at[mine], incoming[c].at[mine], own_sem.at[c])

    def x_copy(c, d):
        part = params.at[:, pl.ds(my_tensor * columns + starts[c], chunks[c])]
        return pltpu.make_async_remote_copy(
            src_ref=part,
            dst_ref=part,
            send_sem=x_send.at[c, d],
            recv_sem=x_recv.at[c, d],
            device_id={"tensor": lax.rem(my_tensor + d, tensors)},
            device_id_type=MESH,
        )

    barrier = pltpu.get_barrier_semaphore()
    axes = (("replica", my_replica, replicas), ("expert", my_expert, experts), ("tensor", my_tensor, tensors))
    for axis, mine, size in axes:
        for d in range(1, size):
            pl.semaphore_signal(
                barrier, inc=1, device_id={axis: lax.rem(mine + d, size)}, device_id_type=MESH
            )
    for c in range(count):
        for d in list(range(1, replicas)) + [0]:
            load(c, d).start()
    states = [
        pltpu.make_async_copy(source, held, state_sem.at[i])
        for i, (source, held) in enumerate(
            ((master_params, master), (first_moment, first), (second_moment, second))
        )
    ]
    for copy in states:
        copy.start()

    def note_order(e, carry):
        seen = jnp.int32(0)
        found = [jnp.int32(0)] * pairs
        for j in range(blocks):
            owned = lax.div(block_map[my_expert * blocks + j], jnp.int32(blocks)) == e
            for k in range(pairs):
                found[k] = jnp.where(owned, jnp.where(seen == k, j, found[k]), found[k])
            seen = seen + jnp.where(owned, 1, 0)
        for k in range(pairs):
            order[e * pairs + k] = found[k]
        return carry

    def note_slots(i, carry):
        seen = jnp.int32(0)
        found = [jnp.int32(0)] * pairs
        for j in range(blocks):
            slot = block_map[i * blocks + j] - my_expert * blocks
            owned = jnp.where(slot >= 0, jnp.where(slot < blocks, 1, 0), 0)
            for k in range(pairs):
                found[k] = jnp.where(owned == 1, jnp.where(seen == k, slot, found[k]), found[k])
            seen = seen + owned
        for k in range(pairs):
            slots[i * pairs + k] = found[k]
        return carry

    def note_places(s, carry):
        place = jnp.int32(0)
        for q in range(blocks):
            place = jnp.where(slots[q] == s, q, place)
        places[s] = place
        return carry

    lax.fori_loop(0, experts, note_order, 0)
    lax.fori_loop(0, experts, note_slots, 0)
    lax.fori_loop(0, blocks, note_places, 0)

    pl.semaphore_wait(barrier, replicas + experts + tensors - 3)
    for c in range(count):
        for d in range(1, replicas):
            load(c, d).wait()
            y_copy(c, d).start()

    shares = [
        1.0 / jnp.full((8, LANES), 1 + step_offsets[lax.rem(my_replica + replicas - d, replicas)], jnp.int32).astype(jnp.float32)
        for d in range(replicas)
    ]
    total = functools.reduce(lambda a, b: a + b, shares)
    weights = [(share / total)[:1] for share in shares]

    fix_one = 1.0 - beta_one**outer_round
    fix_two = 1.0 - beta_two**outer_round

    def add_up(c):
        load(c, 0).wait()
        for d in range(1, replicas):
            y_copy(c, d).wait_recv()
        dense = chunks[c] * rows
        own = stage[c].reshape(replicas, blocks, dense, LANES)
        others = arrived[c].reshape(replicas - 1, blocks, dense, LANES)
        out = outgoing[c].reshape(blocks, dense, LANES)

        def step(n, carry):
            for u in range(UNROLL):
                p = n * UNROLL + u
                block = order[p]
                value = own[0, block].astype(jnp.float32) * weights[0]
                for d in range(1, replicas):
                    value = value + others[d - 1, block].astype(jnp.float32) * weights[d]
                out[p] = value.astype(jnp.bfloat16)
            return carry

        lax.fori_loop(0, blocks // UNROLL, step, 0)

    def adam(c):
        dense = chunks[c] * rows
        terms = incoming[c].reshape(blocks, dense, LANES)
        held = params.reshape(blocks, tensors * columns * rows, LANES)
        part = pl.ds(starts[c] * rows, dense)
        target = pl.ds(pl.multiple_of((my_tensor * columns + starts[c]) * rows, 16), dense)

        def step(n, carry):
            for u in range(UNROLL):
                s = n * UNROLL + u
                gradient = terms[places[s]].astype(jnp.float32)
                one = beta_one * first[s, part] + (1.0 - beta_one) * gradient
                two = beta_two * second[s, part] + (1.0 - beta_two) * gradient * gradient
                new_first[s, part] = one
                new_second[s, part] = two
                update = (outer_rate / fix_one) * one / (jnp.sqrt(two * (1.0 / fix_two)) + epsilon)
                held[s, target] = (master[s, part] - update).astype(jnp.bfloat16)
            return carry

        lax.fori_loop(0, blocks // UNROLL, step, 0)

    def finish(c):
        if c == 0:
            for copy in states:
                copy.wait()
        z_own(c).wait()
        for d in range(1, experts):
            z_copy(c, d).wait_recv()
        adam(c)
        for d in range(1, tensors):
            x_copy(c, d).start()

    for c in range(count):
        add_up(c)
        for d in range(1, experts):
            z_copy(c, d).start()
        z_own(c).start()
        if c >= LAG:
            finish(c - LAG)
    for c in range(max(count - LAG, 0), count):
        finish(c)

    for c in range(count):
        for d in range(1, replicas):
            y_copy(c, d).wait_send()
        for d in range(1, experts):
            z_copy(c, d).wait_send()
    for c in range(count):
        for d in range(1, tensors):
            x_copy(c, d).wait()


def write_out(*refs):
    half = (len(refs) - 1) // 2
    sems = refs[-1]
    copies = [
        pltpu.make_async_copy(refs[i], refs[half + i], sems.at[i])
        for i in range(half)
    ]
    for copy in copies:
        copy.start()
    for copy in copies:
        copy.wait()


def body(delta, step_offsets, block_map, master_params, first_moment, second_moment, *, shape):
    replicas, experts, tensors = shape
    blocks, rows_all, width = delta.shape[1:]
    rows = rows_all // replicas
    columns = width // LANES
    pairs = blocks // experts
    chunks = [CHUNK] * (columns // CHUNK)
    count = len(chunks)
    terms = delta.reshape(blocks, replicas, rows, columns, LANES).transpose(0, 3, 1, 2, 4)

    def dense(state):
        split = state.reshape(blocks, rows, columns, LANES).transpose(0, 2, 1, 3)
        return split.reshape(blocks, columns * rows, LANES)

    def undense(state):
        split = state.reshape(blocks, columns, rows, LANES).transpose(0, 2, 1, 3)
        return split.reshape(blocks, rows, width)

    state_shape = (blocks, columns * rows, LANES)
    params_shape = (blocks, tensors * columns, rows, LANES)
    anywhere = pl.BlockSpec(memory_space=pltpu.HBM)
    near = pl.BlockSpec(memory_space=pltpu.VMEM)
    scalars = pl.BlockSpec(memory_space=pltpu.SMEM)
    dma = pltpu.SemaphoreType.DMA
    sizes = (replicas, experts, tensors, chunks, blocks, pairs, rows)
    held = pl.pallas_call(
        functools.partial(kernel, sizes),
        out_shape=(
            pltpu.VMEM(params_shape, jnp.bfloat16),
            pltpu.VMEM(state_shape, jnp.float32),
            pltpu.VMEM(state_shape, jnp.float32),
        ),
        in_specs=[scalars] * 2 + [anywhere] * 4,
        out_specs=(near,) * 3,
        scratch_shapes=[
            pltpu.VMEM(state_shape, jnp.float32),
            pltpu.VMEM(state_shape, jnp.float32),
            pltpu.VMEM(state_shape, jnp.float32),
            pltpu.SMEM((blocks,), jnp.int32),
            pltpu.SMEM((blocks,), jnp.int32),
            pltpu.SMEM((blocks,), jnp.int32),
            dma((count, replicas)),
            dma((3,)),
            dma((count,)),
            dma((count, replicas)),
            dma((count, replicas)),
            dma((count, experts)),
            dma((count, experts)),
            dma((count, tensors)),
            dma((count, tensors)),
        ]
        + [pltpu.VMEM((replicas, blocks, c, rows, LANES), jnp.bfloat16) for c in chunks]
        + [pltpu.VMEM((replicas - 1, blocks, c, rows, LANES), jnp.bfloat16) for c in chunks]
        + [pltpu.VMEM((blocks, c, rows, LANES), jnp.bfloat16) for c in chunks]
        + [pltpu.VMEM((blocks, c, rows, LANES), jnp.bfloat16) for c in chunks],
        compiler_params=pltpu.CompilerParams(collective_id=0, has_side_effects=True),
    )(block_map, step_offsets, terms, dense(master_params), dense(first_moment), dense(second_moment))
    new_params, new_first, new_second = pl.pallas_call(
        write_out,
        out_shape=(
            jax.ShapeDtypeStruct(params_shape, jnp.bfloat16),
            jax.ShapeDtypeStruct(state_shape, jnp.float32),
            jax.ShapeDtypeStruct(state_shape, jnp.float32),
        ),
        in_specs=[near] * 3,
        out_specs=(anywhere,) * 3,
        scratch_shapes=[dma((3,))],
        compiler_params=pltpu.CompilerParams(vmem_limit_bytes=1024 * 1024),
    )(*held)
    full = new_params.transpose(0, 2, 1, 3).reshape(blocks, rows, tensors * width)
    return (full, undense(new_first), undense(new_second))


def solution(mesh):
    in_specs = (
        P("replica", "expert", None, "tensor"),
        P(),
        P(),
        P("expert", "replica", "tensor"),
        P("expert", "replica", "tensor"),
        P("expert", "replica", "tensor"),
    )
    out_specs = (
        P("expert", "replica", None),
        P("expert", "replica", "tensor"),
        P("expert", "replica", "tensor"),
    )
    shape = tuple(mesh.shape[axis] for axis in ("replica", "expert", "tensor"))
    step = functools.partial(body, shape=shape)
    return jax.shard_map(step, mesh=mesh, in_specs=in_specs, out_specs=out_specs, check_vma=False)
```

```python
import functools

import jax
import jax.numpy as jnp
from jax import lax
from jax.experimental import pallas as pl
from jax.experimental.pallas import tpu as pltpu
from jax.sharding import PartitionSpec as P

beta_one = 0.9
beta_two = 0.99
outer_rate = 0.7
outer_round = 20
epsilon = 1e-08

LANES = 128
CHUNK = 8
LAG = 2
UNROLL = 16
MESH = pl.DeviceIdType.MESH


def kernel(
    sizes,
    block_map,
    step_offsets,
    delta,
    master_params,
    first_moment,
    second_moment,
    params,
    new_first,
    new_second,
    master,
    first,
    second,
    order,
    slots,
    places,
    load_sem,
    state_sem,
    own_sem,
    y_send,
    y_recv,
    z_send,
    z_recv,
    x_send,
    x_recv,
    *buffers,
):
    replicas, experts, tensors, chunks, blocks, pairs, rows = sizes
    count = len(chunks)
    stage = buffers[:count]
    arrived = buffers[count : 2 * count]
    outgoing = buffers[2 * count : 3 * count]
    incoming = buffers[3 * count :]
    my_replica = lax.axis_index("replica")
    my_expert = lax.axis_index("expert")
    my_tensor = lax.axis_index("tensor")
    columns = sum(chunks)
    starts = [sum(chunks[:c]) for c in range(count)]

    def load(c, d):
        replica = lax.rem(my_replica + d, replicas)
        return pltpu.make_async_copy(
            delta.at[:, pl.ds(starts[c], chunks[c]), replica],
            stage[c].at[d],
            load_sem.at[c, d],
        )

    def y_copy(c, d):
        return pltpu.make_async_remote_copy(
            src_ref=stage[c].at[d],
            dst_ref=arrived[c].at[d - 1],
            send_sem=y_send.at[c, d],
            recv_sem=y_recv.at[c, d],
            device_id={"replica": lax.rem(my_replica + d, replicas)},
            device_id_type=MESH,
        )

    def z_copy(c, d):
        peer = lax.rem(my_expert + d, experts)
        return pltpu.make_async_remote_copy(
            src_ref=outgoing[c].at[pl.ds(peer * pairs, pairs)],
            dst_ref=incoming[c].at[pl.ds(my_expert * pairs, pairs)],
            send_sem=z_send.at[c, d],
            recv_sem=z_recv.at[c, d],
            device_id={"expert": peer},
            device_id_type=MESH,
        )

    def z_own(c):
        mine = pl.ds(my_expert * pairs, pairs)
        return pltpu.make_async_copy(outgoing[c].at[mine], incoming[c].at[mine], own_sem.at[c])

    def x_copy(c, d):
        part = params.at[:, pl.ds(my_tensor * columns + starts[c], chunks[c])]
        return pltpu.make_async_remote_copy(
            src_ref=part,
            dst_ref=part,
            send_sem=x_send.at[c, d],
            recv_sem=x_recv.at[c, d],
            device_id={"tensor": lax.rem(my_tensor + d, tensors)},
            device_id_type=MESH,
        )

    barrier = pltpu.get_barrier_semaphore()
    axes = (("replica", my_replica, replicas), ("expert", my_expert, experts), ("tensor", my_tensor, tensors))
    for axis, mine, size in axes:
        for d in range(1, size):
            pl.semaphore_signal(
                barrier, inc=1, device_id={axis: lax.rem(mine + d, size)}, device_id_type=MESH
            )
    for c in range(count):
        for d in list(range(1, replicas)) + [0]:
            load(c, d).start()
    states = [
        pltpu.make_async_copy(source, held, state_sem.at[i])
        for i, (source, held) in enumerate(
            ((master_params, master), (first_moment, first), (second_moment, second))
        )
    ]
    for copy in states:
        copy.start()

    def note_order(e, carry):
        seen = jnp.int32(0)
        found = [jnp.int32(0)] * pairs
        for j in range(blocks):
            owned = lax.div(block_map[my_expert * blocks + j], jnp.int32(blocks)) == e
            for k in range(pairs):
                found[k] = jnp.where(owned, jnp.where(seen == k, j, found[k]), found[k])
            seen = seen + jnp.where(owned, 1, 0)
        for k in range(pairs):
            order[e * pairs + k] = found[k]
        return carry

    def note_slots(i, carry):
        seen = jnp.int32(0)
        found = [jnp.int32(0)] * pairs
        for j in range(blocks):
            slot = block_map[i * blocks + j] - my_expert * blocks
            owned = jnp.where(slot >= 0, jnp.where(slot < blocks, 1, 0), 0)
            for k in range(pairs):
                found[k] = jnp.where(owned == 1, jnp.where(seen == k, slot, found[k]), found[k])
            seen = seen + owned
        for k in range(pairs):
            slots[i * pairs + k] = found[k]
        return carry

    def note_places(s, carry):
        place = jnp.int32(0)
        for q in range(blocks):
            place = jnp.where(slots[q] == s, q, place)
        places[s] = place
        return carry

    lax.fori_loop(0, experts, note_order, 0)
    lax.fori_loop(0, experts, note_slots, 0)
    lax.fori_loop(0, blocks, note_places, 0)

    pl.semaphore_wait(barrier, replicas + experts + tensors - 3)
    for c in range(count):
        for d in range(1, replicas):
            load(c, d).wait()
            y_copy(c, d).start()

    shares = [
        1.0 / jnp.full((8, LANES), 1 + step_offsets[lax.rem(my_replica + replicas - d, replicas)], jnp.int32).astype(jnp.float32)
        for d in range(replicas)
    ]
    total = functools.reduce(lambda a, b: a + b, shares)
    weights = [(share / total)[:1] for share in shares]

    fix_one = 1.0 - beta_one**outer_round
    fix_two = 1.0 - beta_two**outer_round

    def add_up(c):
        load(c, 0).wait()
        for d in range(1, replicas):
            y_copy(c, d).wait_recv()
        dense = chunks[c] * rows
        own = stage[c].reshape(replicas, blocks, dense, LANES)
        others = arrived[c].reshape(replicas - 1, blocks, dense, LANES)
        out = outgoing[c].reshape(blocks, dense, LANES)

        def step(n, carry):
            for u in range(UNROLL):
                p = n * UNROLL + u
                block = order[p]
                value = own[0, block].astype(jnp.float32) * weights[0]
                for d in range(1, replicas):
                    value = value + others[d - 1, block].astype(jnp.float32) * weights[d]
                out[p] = value.astype(jnp.bfloat16)
            return carry

        lax.fori_loop(0, blocks // UNROLL, step, 0)

    def adam(c):
        dense = chunks[c] * rows
        terms = incoming[c].reshape(blocks, dense, LANES)
        held = params.reshape(blocks, tensors * columns * rows, LANES)
        part = pl.ds(starts[c] * rows, dense)
        target = pl.ds(pl.multiple_of((my_tensor * columns + starts[c]) * rows, 16), dense)

        def step(n, carry):
            for u in range(UNROLL):
                s = n * UNROLL + u
                gradient = terms[places[s]].astype(jnp.float32)
                one = beta_one * first[s, part] + (1.0 - beta_one) * gradient
                two = beta_two * second[s, part] + (1.0 - beta_two) * gradient * gradient
                new_first[s, part] = one
                new_second[s, part] = two
                update = (outer_rate / fix_one) * one / (jnp.sqrt(two * (1.0 / fix_two)) + epsilon)
                held[s, target] = (master[s, part] - update).astype(jnp.bfloat16)
            return carry

        lax.fori_loop(0, blocks // UNROLL, step, 0)

    def finish(c):
        if c == 0:
            for copy in states:
                copy.wait()
        z_own(c).wait()
        for d in range(1, experts):
            z_copy(c, d).wait_recv()
        adam(c)
        for d in range(1, tensors):
            x_copy(c, d).start()

    for c in range(count):
        add_up(c)
        for d in range(1, experts):
            z_copy(c, d).start()
        z_own(c).start()
        if c >= LAG:
            finish(c - LAG)
    for c in range(max(count - LAG, 0), count):
        finish(c)

    for c in range(count):
        for d in range(1, replicas):
            y_copy(c, d).wait_send()
        for d in range(1, experts):
            z_copy(c, d).wait_send()
    for c in range(count):
        for d in range(1, tensors):
            x_copy(c, d).wait()


def write_out(*refs):
    half = (len(refs) - 1) // 2
    sems = refs[-1]
    copies = [
        pltpu.make_async_copy(refs[i], refs[half + i], sems.at[i])
        for i in range(half)
    ]
    for copy in copies:
        copy.start()
    for copy in copies:
        copy.wait()


def body(delta, step_offsets, block_map, master_params, first_moment, second_moment, *, shape):
    replicas, experts, tensors = shape
    blocks, rows_all, width = delta.shape[1:]
    rows = rows_all // replicas
    columns = width // LANES
    pairs = blocks // experts
    chunks = [CHUNK] * (columns // CHUNK)
    count = len(chunks)
    terms = delta.reshape(blocks, replicas, rows, columns, LANES).transpose(0, 3, 1, 2, 4)

    def dense(state):
        split = state.reshape(blocks, rows, columns, LANES).transpose(0, 2, 1, 3)
        return split.reshape(blocks, columns * rows, LANES)

    def undense(state):
        split = state.reshape(blocks, columns, rows, LANES).transpose(0, 2, 1, 3)
        return split.reshape(blocks, rows, width)

    state_shape = (blocks, columns * rows, LANES)
    params_shape = (blocks, tensors * columns, rows, LANES)
    anywhere = pl.BlockSpec(memory_space=pltpu.HBM)
    near = pl.BlockSpec(memory_space=pltpu.VMEM)
    scalars = pl.BlockSpec(memory_space=pltpu.SMEM)
    dma = pltpu.SemaphoreType.DMA
    sizes = (replicas, experts, tensors, chunks, blocks, pairs, rows)
    held = pl.pallas_call(
        functools.partial(kernel, sizes),
        out_shape=(
            pltpu.VMEM(params_shape, jnp.bfloat16),
            pltpu.VMEM(state_shape, jnp.float32),
            pltpu.VMEM(state_shape, jnp.float32),
        ),
        in_specs=[scalars] * 2 + [anywhere] * 4,
        out_specs=(near,) * 3,
        scratch_shapes=[
            pltpu.VMEM(state_shape, jnp.float32),
            pltpu.VMEM(state_shape, jnp.float32),
            pltpu.VMEM(state_shape, jnp.float32),
            pltpu.SMEM((blocks,), jnp.int32),
            pltpu.SMEM((blocks,), jnp.int32),
            pltpu.SMEM((blocks,), jnp.int32),
            dma((count, replicas)),
            dma((3,)),
            dma((count,)),
            dma((count, replicas)),
            dma((count, replicas)),
            dma((count, experts)),
            dma((count, experts)),
            dma((count, tensors)),
            dma((count, tensors)),
        ]
        + [pltpu.VMEM((replicas, blocks, c, rows, LANES), jnp.bfloat16) for c in chunks]
        + [pltpu.VMEM((replicas - 1, blocks, c, rows, LANES), jnp.bfloat16) for c in chunks]
        + [pltpu.VMEM((blocks, c, rows, LANES), jnp.bfloat16) for c in chunks]
        + [pltpu.VMEM((blocks, c, rows, LANES), jnp.bfloat16) for c in chunks],
        compiler_params=pltpu.CompilerParams(collective_id=0, has_side_effects=True),
    )(block_map, step_offsets, terms, dense(master_params), dense(first_moment), dense(second_moment))
    new_params, new_first, new_second = pl.pallas_call(
        write_out,
        out_shape=(
            jax.ShapeDtypeStruct(params_shape, jnp.bfloat16),
            jax.ShapeDtypeStruct(state_shape, jnp.float32),
            jax.ShapeDtypeStruct(state_shape, jnp.float32),
        ),
        in_specs=[near] * 3,
        out_specs=(anywhere,) * 3,
        scratch_shapes=[dma((3,))],
        compiler_params=pltpu.CompilerParams(vmem_limit_bytes=1024 * 1024),
    )(*held)
    full = new_params.transpose(0, 2, 1, 3).reshape(blocks, rows, tensors * width)
    return (full, undense(new_first), undense(new_second))


def solution(mesh):
    in_specs = (
        P("replica", "expert", None, "tensor"),
        P(),
        P(),
        P("expert", "replica", "tensor"),
        P("expert", "replica", "tensor"),
        P("expert", "replica", "tensor"),
    )
    out_specs = (
        P("expert", "replica", None),
        P("expert", "replica", "tensor"),
        P("expert", "replica", "tensor"),
    )
    shape = tuple(mesh.shape[axis] for axis in ("replica", "expert", "tensor"))
    step = functools.partial(body, shape=shape)
    return jax.shard_map(step, mesh=mesh, in_specs=in_specs, out_specs=out_specs, check_vma=False)
```
